128 devices in a mesh: tp: 4 (over x), sp: 32 (over z, y, core).
Axes of the slice: x: 4, y: 4, z: 4, core: 2. Of those that a mesh axis runs over, the one named last changes fastest.
Arguments:
- x: bfloat16 [8, 4096], replicated
- seq_len: int32 [8], replicated
- ln_w: bfloat16 [4096], replicated
- w_q: bfloat16 [4096, 4096], P(None, 'tp')
- w_o: bfloat16 [4096, 4096], P('tp')
- w_gate: bfloat16 [4096, 14336], P(None, 'tp')
- w_up: bfloat16 [4096, 14336], P(None, 'tp')
- w_down: bfloat16 [14336, 4096], P('tp')
- k_cache: bfloat16 [8, 8, 32768, 128], P(None, 'tp', 'sp')
- v_cache: bfloat16 [8, 8, 32768, 128], P(None, 'tp', 'sp')
Outputs:
- output: bfloat16 [8, 4096], replicated
All inputs are finite; a program needn't handle non-finite values.
Results may differ from the reference program's by a relative error of at most 0.00718116.
Values sent between devices are 32-bit elements.
A program may use at most 1 GiB of HBM per device.

```python
import jax
import jax.numpy as jnp
from jax import lax

BATCH_ROWS = 8
HIDDEN = 4096
Q_HEADS = 32
KV_HEADS = 8
HEAD_DIM = 128
FFN_DIM = 14336
SEQ_LEN = 32768
LN_EPS = 1e-5


def setup_inputs(seed: int = 0) -> dict:
    keys = jax.random.split(jax.random.key(seed), 10)
    q_width = Q_HEADS * HEAD_DIM
    cache_shape = (BATCH_ROWS, KV_HEADS, SEQ_LEN, HEAD_DIM)
    out_scale = (SEQ_LEN / 16.0) ** 0.5 * q_width ** -0.5

    def normal_draw(rng_key, shape, scale):
        return (jax.random.normal(rng_key, shape, jnp.float32) * scale).astype(jnp.bfloat16)

    seq_len = jax.random.randint(keys[1], (BATCH_ROWS,), SEQ_LEN // 2, SEQ_LEN, jnp.int32)
    seq_len = seq_len.at[0].set(SEQ_LEN - 1)
    ln_w = (1.0 + 0.3 * jax.random.normal(keys[2], (HIDDEN,), jnp.float32)).astype(jnp.bfloat16)
    return {
        'x': normal_draw(keys[0], (BATCH_ROWS, HIDDEN), 1.0),
        'seq_len': seq_len,
        'ln_w': ln_w,
        'w_q': normal_draw(keys[3], (HIDDEN, q_width), HIDDEN ** -0.5),
        'w_o': normal_draw(keys[4], (q_width, HIDDEN), out_scale),
        'w_gate': normal_draw(keys[5], (HIDDEN, FFN_DIM), HIDDEN ** -0.5),
        'w_up': normal_draw(keys[6], (HIDDEN, FFN_DIM), HIDDEN ** -0.5),
        'w_down': normal_draw(keys[7], (FFN_DIM, HIDDEN), FFN_DIM ** -0.5),
        'k_cache': normal_draw(keys[8], cache_shape, 1.5),
        'v_cache': normal_draw(keys[9], cache_shape, 1.0),
    }


def layer_norm(x, ln_w):
    x_f32 = x.astype(jnp.float32)
    centered = x_f32 - jnp.mean(x_f32, axis=-1, keepdims=True)
    variance = jnp.mean(centered * centered, axis=-1, keepdims=True)
    return (centered * lax.rsqrt(variance + LN_EPS) * ln_w.astype(jnp.float32)).astype(jnp.bfloat16)


def reference(x, seq_len, ln_w, w_q, w_o, w_gate, w_up, w_down, k_cache, v_cache):
    group_size = Q_HEADS // KV_HEADS
    hidden = layer_norm(x, ln_w)
    query = jnp.dot(hidden, w_q, preferred_element_type=jnp.float32).astype(jnp.bfloat16)
    positions = jnp.arange(SEQ_LEN)

    def attend(operands):
        q_rows, k_rows, v_rows, length = operands
        scores = jnp.dot(q_rows.astype(jnp.float32), k_rows.astype(jnp.float32).T) * HEAD_DIM ** -0.5
        scores = jnp.where(positions[None, :] <= length, scores, -jnp.inf)
        probs = jax.nn.softmax(scores, axis=-1)
        return jnp.dot(probs, v_rows.astype(jnp.float32))

    attn_heads = lax.map(attend, (
        query.reshape(BATCH_ROWS * KV_HEADS, group_size, HEAD_DIM),
        k_cache.reshape(BATCH_ROWS * KV_HEADS, SEQ_LEN, HEAD_DIM),
        v_cache.reshape(BATCH_ROWS * KV_HEADS, SEQ_LEN, HEAD_DIM),
        jnp.repeat(seq_len, KV_HEADS)))
    attn_vals = attn_heads.reshape(BATCH_ROWS, Q_HEADS * HEAD_DIM).astype(jnp.bfloat16)
    attn_proj = jnp.dot(attn_vals, w_o, preferred_element_type=jnp.float32)
    gate_proj = jnp.dot(hidden, w_gate, preferred_element_type=jnp.float32)
    up_proj = jnp.dot(hidden, w_up, preferred_element_type=jnp.float32)
    act_vals = (jax.nn.silu(gate_proj) * up_proj).astype(jnp.bfloat16)
    mlp_proj = jnp.dot(act_vals, w_down, preferred_element_type=jnp.float32)
    x_out = (x.astype(jnp.float32) + attn_proj + mlp_proj).astype(jnp.bfloat16)
    return x_out
```

```python
import functools

import jax
import jax.numpy as jnp
from jax import lax
from jax.experimental import pallas as pl
from jax.experimental.pallas import tpu as pltpu
from jax.sharding import PartitionSpec as P

LN_EPS = 1e-5
NEG_BIG = -1e30
LOG2E = 1.4426950408889634
MESH = pl.DeviceIdType.MESH
F32 = jnp.float32
BF16 = jnp.bfloat16

ROWS = 8
HID = 4096
HD = 128
BLK = 1024
FF_BLOCKS = 28
WQ_CHUNKS = 4


def kernel(x_hbm, len_hbm, lnw_hbm, wq_hbm, wo_hbm, wg_hbm, wu_hbm, wd_hbm, k_hbm, v_hbm, out_ref,
           x_v, lnw_v, len_s, wq_v, wg_v, wu_v, k_v, v_v, wo_v, wd_v,
           q_b, mz_b, mg_b, ds_b, dr_b, y_b, z_b, of_b, xs_b, g_b,
           in_sem, wq_sem, gu_sem, k_sem, v_sem, w2_sem,
           q_ss, q_rs, mz_ss, mz_rs, mg_ss, mg_rs, d_ss, d_rs, y_ss, y_rs, z_ss, z_rs, x_ss, x_rs, g_ss, g_rs):
    xi = lax.axis_index('tp')
    sp = lax.axis_index('sp')
    c = lax.rem(sp, 2)
    y = lax.rem(lax.div(sp, 2), 4)
    z = lax.div(sp, 8)
    oc = 1 - c
    grp = y * 2 + c

    def dev(x_, z_, y_, c_):
        return (x_, (z_ * 4 + y_) * 2 + c_)

    def up(v, k):
        return lax.rem(v + k, 4)

    partner = dev(xi, z, y, oc)
    z_peers = [dev(xi, up(z, k), y, c) for k in (1, 2, 3)]
    y_peers = [dev(xi, z, up(y, k), c) for k in (1, 2, 3)]
    x_peers = [dev(up(xi, k), z, y, c) for k in (1, 2, 3)]
    yo_peers = [dev(xi, z, up(y, k), oc) for k in (1, 2, 3)]

    bar = pltpu.get_barrier_semaphore()
    everyone = [partner] + z_peers + y_peers + x_peers + yo_peers
    for d in everyone:
        pl.semaphore_signal(bar, inc=1, device_id=d, device_id_type=MESH)

    def start(src, dst, sem):
        cp = pltpu.make_async_copy(src, dst, sem)
        cp.start()
        return cp

    cp_x = start(x_hbm, x_v, in_sem.at[0])
    cp_lnw = start(lnw_hbm, lnw_v, in_sem.at[1])
    cp_len = start(len_hbm, len_s, in_sem.at[2])
    kc = HID // WQ_CHUNKS
    cp_wq = [start(wq_hbm.at[pl.ds(i * kc, kc), pl.ds(pl.multiple_of(c * 512, 512), 512)], wq_v.at[i], wq_sem.at[i])
             for i in range(WQ_CHUNKS)]
    ff = pl.multiple_of(jnp.minimum(z * 8 + grp, FF_BLOCKS - 1) * 128, 128)
    cp_g = start(wg_hbm.at[:, pl.ds(ff, 128)], wg_v, gu_sem.at[0])
    cp_u = start(wu_hbm.at[:, pl.ds(ff, 128)], wu_v, gu_sem.at[1])

    def row_of(j):
        return 4 * oc + j if j < 4 else 4 * c + (j - 4)

    cp_k, cp_v = [], []
    for j in range(8):
        cp_k.append(start(k_hbm.at[row_of(j)], k_v.at[j], k_sem.at[j]))
        cp_v.append(start(v_hbm.at[row_of(j)], v_v.at[j], v_sem.at[j]))
    cols = pl.ds(pl.multiple_of(y * 1024, 1024), 1024)
    cp_wo = start(wo_hbm.at[:, cols], wo_v, w2_sem.at[0])
    cp_wd = start(wd_hbm.at[:, cols], wd_v, w2_sem.at[1])

    sends = []

    def send(src, dst, ss, rs, d):
        cp = pltpu.make_async_remote_copy(src_ref=src, dst_ref=dst, send_sem=ss, recv_sem=rs,
                                          device_id=d, device_id_type=MESH)
        cp.start()
        sends.append(cp)

    def recv(dst, ss, rs, d):
        pltpu.make_async_remote_copy(src_ref=dst, dst_ref=dst, send_sem=ss, recv_sem=rs,
                                     device_id=d, device_id_type=MESH).wait_recv()

    cp_x.wait()
    cp_lnw.wait()
    xf = x_v[...].astype(F32)
    cen = xf - jnp.mean(xf, axis=-1, keepdims=True)
    var = jnp.mean(cen * cen, axis=-1, keepdims=True)
    h = (cen * lax.rsqrt(var + LN_EPS) * lnw_v[...].astype(F32).reshape(1, HID)).astype(BF16)

    q = jnp.zeros((ROWS, 512), F32)
    for i in range(WQ_CHUNKS):
        cp_wq[i].wait()
        q = q + jnp.dot(h[:, i * kc:(i + 1) * kc], wq_v[i], preferred_element_type=F32)
    q = q.astype(BF16).astype(F32)
    qrows = pl.ds(pl.multiple_of(c * 32, 32), 32)
    q_b[qrows, :] = jnp.concatenate([q[:, i * HD:(i + 1) * HD] for i in range(4)], axis=0)
    pl.semaphore_wait(bar, len(everyone))
    send(q_b.at[qrows, :], q_b.at[qrows, :], q_ss.at[0], q_rs.at[0], partner)

    cp_g.wait()
    cp_u.wait()
    gu = jnp.dot(h, jnp.concatenate([wg_v[...], wu_v[...]], axis=1), preferred_element_type=F32)
    act = (jax.nn.silu(gu[:, :HD]) * gu[:, HD:]).astype(BF16).astype(F32)
    mz_b[z] = act
    for k in (1, 2, 3):
        send(mz_b.at[z], mz_b.at[z], mz_ss.at[k - 1], mz_rs.at[z], z_peers[k - 1])

    prow = pl.ds(pl.multiple_of(oc * 32, 32), 32)
    recv(q_b.at[prow, :], q_ss.at[0], q_rs.at[0], partner)
    cp_len.wait()
    lane = lax.broadcasted_iota(jnp.int32, (ROWS, HD), 1)
    top = lax.broadcasted_iota(jnp.int32, (ROWS, HD), 0) < 4
    pos = sp * BLK + lax.broadcasted_iota(jnp.int32, (ROWS, BLK), 1)
    cs = (HD ** -0.5) * LOG2E

    def attend(j):
        b = row_of(j)
        qh = q_b[pl.ds(b, 8, stride=8), :]
        qd = jnp.concatenate([jnp.where(top, qh, 0.0), jnp.where(top, 0.0, qh)], axis=1).astype(BF16)
        cp_k[j].wait()
        kk = jnp.concatenate([k_v[j, 0], k_v[j, 1]], axis=1)
        s = lax.dot_general(qd, kk, (((1,), (1,)), ((), ())), preferred_element_type=F32)
        s = jnp.where(pos <= len_s[b], s, -jnp.inf)
        m = jnp.maximum(jnp.max(s, axis=-1, keepdims=True), NEG_BIG)
        p = jnp.exp2((s - m) * cs)
        l = jnp.sum(p, axis=-1, keepdims=True)
        cp_v[j].wait()
        vv = jnp.concatenate([v_v[j, 0], v_v[j, 1]], axis=1)
        o2 = jnp.dot(p.astype(BF16), vv, preferred_element_type=F32)
        return jnp.where(top, o2[:, :HD], o2[:, HD:]), m, l

    def stats_tile(ms, ls):
        t = jnp.zeros((ROWS, HD), F32)
        for i in range(4):
            t = jnp.where(lane == i, ms[i], t)
            t = jnp.where(lane == 4 + i, ls[i], t)
        return t

    ms, ls = [], []
    for j in range(4):
        o, m, l = attend(j)
        ds_b[j] = o
        ms.append(m)
        ls.append(l)
    ds_b[4] = stats_tile(ms, ls)
    send(ds_b, dr_b, d_ss.at[0], d_rs.at[0], partner)
    own = [attend(j) for j in range(4, 8)]

    def combine(parts):
        mx = functools.reduce(jnp.maximum, [p[1] for p in parts])
        ws = [jnp.exp2((p[1] - mx) * cs) for p in parts]
        o = functools.reduce(jnp.add, [p[0] * w for p, w in zip(parts, ws)])
        l = functools.reduce(jnp.add, [p[2] * w for p, w in zip(parts, ws)])
        return o, mx, l

    def unpack(tile_of, i, st):
        return tile_of(i), st[:, i:i + 1], st[:, 4 + i:5 + i]

    recv(dr_b, d_ss.at[0], d_rs.at[0], partner)
    st = dr_b[4]
    ms, ls = [], []
    for i in range(4):
        o, m, l = combine([own[i], unpack(lambda r: dr_b[r], i, st)])
        y_b[y, i] = o
        ms.append(m)
        ls.append(l)
    y_b[y, 4] = stats_tile(ms, ls)
    for k in (1, 2, 3):
        send(y_b.at[y], y_b.at[y], y_ss.at[k - 1], y_rs.at[y], y_peers[k - 1])

    for k in (1, 2, 3):
        recv(mz_b.at[up(z, k)], mz_ss.at[k - 1], mz_rs.at[up(z, k)], z_peers[k - 1])
    mg_b[grp] = mz_b[...]
    gpeers = ([(partner, y * 2 + oc)] + [(y_peers[k - 1], up(y, k) * 2 + c) for k in (1, 2, 3)]
              + [(yo_peers[k - 1], up(y, k) * 2 + oc) for k in (1, 2, 3)])
    for n, (d, _) in enumerate(gpeers):
        send(mz_b, mg_b.at[grp], mg_ss.at[n], mg_rs.at[grp], d)

    for k in (1, 2, 3):
        recv(y_b.at[up(y, k)], y_ss.at[k - 1], y_rs.at[up(y, k)], y_peers[k - 1])
    ms, ls = [], []
    sts = [y_b[n, 4] for n in range(4)]
    for i in range(4):
        o, m, l = combine([unpack(lambda r, n=n: y_b[n, r], i, sts[n]) for n in range(4)])
        z_b[z, i] = o
        ms.append(m)
        ls.append(l)
    z_b[z, 4] = stats_tile(ms, ls)
    for k in (1, 2, 3):
        send(z_b.at[z], z_b.at[z], z_ss.at[k - 1], z_rs.at[z], z_peers[k - 1])

    for n, (d, g) in enumerate(gpeers):
        recv(mg_b.at[g], mg_ss.at[n], mg_rs.at[g], d)
    ml = jnp.concatenate([mg_b[i % 8, i // 8] for i in range(FF_BLOCKS)], axis=1).astype(BF16)
    cp_wd.wait()
    r1 = jnp.dot(ml, wd_v[:, :512], preferred_element_type=F32)
    r2 = jnp.dot(ml, wd_v[:, 512:], preferred_element_type=F32)

    for k in (1, 2, 3):
        recv(z_b.at[up(z, k)], z_ss.at[k - 1], z_rs.at[up(z, k)], z_peers[k - 1])
    sts = [z_b[n, 4] for n in range(4)]
    for i in range(4):
        o, m, l = combine([unpack(lambda r, n=n: z_b[n, r], i, sts[n]) for n in range(4)])
        o = o / l
        of_b[pl.ds(i * 8, 8), :] = o
        of_b[pl.ds(32 + i * 8, 8), :] = o
    ol = jnp.concatenate([of_b[pl.ds(n, 8, stride=8), :] for n in range(8)], axis=1).astype(BF16)
    cp_wo.wait()
    r1 = r1 + jnp.dot(ol, wo_v[:, :512], preferred_element_type=F32)
    r2 = r2 + jnp.dot(ol, wo_v[:, 512:], preferred_element_type=F32)

    upper = lax.broadcasted_iota(jnp.int32, (ROWS, 512), 0) < 4
    keep = jnp.logical_xor(upper, jnp.broadcast_to(c == 1, (ROWS, 512)))
    xs_b[xi] = jnp.where(keep, r1, pltpu.roll(r2, 4, 0))
    for k in (1, 2, 3):
        send(xs_b.at[xi], xs_b.at[xi], x_ss.at[k - 1], x_rs.at[xi], x_peers[k - 1])
    xc = x_v[:, pl.ds(pl.multiple_of(y * 1024, 1024), 1024)].astype(F32)
    xr = jnp.where(keep, xc[:, :512], pltpu.roll(xc[:, 512:], 4, 0))
    for k in (1, 2, 3):
        recv(xs_b.at[up(xi, k)], x_ss.at[k - 1], x_rs.at[up(xi, k)], x_peers[k - 1])
    tot = xr + ((xs_b[0] + xs_b[1]) + (xs_b[2] + xs_b[3]))
    g_b[grp] = tot.astype(BF16).astype(F32)
    for n, (d, _) in enumerate(gpeers):
        send(g_b.at[grp], g_b.at[grp], g_ss.at[n], g_rs.at[grp], d)
    for n, (d, g) in enumerate(gpeers):
        recv(g_b.at[g], g_ss.at[n], g_rs.at[g], d)
    for yy in range(4):
        a0, a1 = g_b[2 * yy], g_b[2 * yy + 1]
        out_ref[:, yy * 1024:yy * 1024 + 512] = jnp.where(upper, a0, a1).astype(BF16)
        out_ref[:, yy * 1024 + 512:yy * 1024 + 1024] = pltpu.roll(jnp.where(upper, a1, a0), 4, 0).astype(BF16)
    for cp in sends:
        cp.wait_send()


def solution(mesh):
    cache_spec = P(None, 'tp', 'sp', None)
    col_spec = P(None, 'tp')
    row_spec = P('tp', None)
    any_spec = pl.BlockSpec(memory_space=pl.ANY)
    dma = pltpu.SemaphoreType.DMA

    def local_step(*args):
        return pl.pallas_call(
            kernel,
            out_shape=jax.ShapeDtypeStruct((ROWS, HID), BF16),
            in_specs=[any_spec] * 10,
            out_specs=pl.BlockSpec(memory_space=pltpu.VMEM),
            scratch_shapes=[
                pltpu.VMEM((ROWS, HID), BF16),
                pltpu.VMEM((HID,), BF16),
                pltpu.SMEM((ROWS,), jnp.int32),
                pltpu.VMEM((WQ_CHUNKS, HID // WQ_CHUNKS, 512), BF16),
                pltpu.VMEM((HID, HD), BF16),
                pltpu.VMEM((HID, HD), BF16),
                pltpu.VMEM((8, 2, BLK, HD), BF16),
                pltpu.VMEM((8, 2, BLK, HD), BF16),
                pltpu.VMEM((1024, 1024), BF16),
                pltpu.VMEM((3584, 1024), BF16),
                pltpu.VMEM((64, HD), F32),
                pltpu.VMEM((4, ROWS, HD), F32),
                pltpu.VMEM((8, 4, ROWS, HD), F32),
                pltpu.VMEM((5, ROWS, HD), F32),
                pltpu.VMEM((5, ROWS, HD), F32),
                pltpu.VMEM((4, 5, ROWS, HD), F32),
                pltpu.VMEM((4, 5, ROWS, HD), F32),
                pltpu.VMEM((64, HD), F32),
                pltpu.VMEM((4, ROWS, 512), F32),
                pltpu.VMEM((8, ROWS, 512), F32),
                dma((3,)), dma((WQ_CHUNKS,)), dma((2,)), dma((8,)), dma((8,)), dma((2,)),
                dma((1,)), dma((1,)),
                dma((3,)), dma((4,)),
                dma((7,)), dma((8,)),
                dma((1,)), dma((1,)),
                dma((3,)), dma((4,)),
                dma((3,)), dma((4,)),
                dma((3,)), dma((4,)),
                dma((7,)), dma((8,)),
            ],
            compiler_params=pltpu.CompilerParams(collective_id=0, has_side_effects=True,
                                                 vmem_limit_bytes=56 * 1024 * 1024),
        )(*args)

    return jax.shard_map(local_step, mesh=mesh,
                         in_specs=(P(), P(), P(), col_spec, row_spec,
                                   col_spec, col_spec, row_spec, cache_spec, cache_spec),
                         out_specs=P(), check_vma=False)
```

```python
import functools

import jax
import jax.numpy as jnp
from jax import lax
from jax.experimental import pallas as pl
from jax.experimental.pallas import tpu as pltpu
from jax.sharding import PartitionSpec as P

LN_EPS = 1e-5
NEG_BIG = -1e30
LOG2E = 1.4426950408889634
MESH = pl.DeviceIdType.MESH
F32 = jnp.float32
BF16 = jnp.bfloat16

ROWS = 8
HID = 4096
HD = 128
BLK = 1024
FF_BLOCKS = 28
WQ_CHUNKS = 4


def kernel(x_hbm, len_hbm, lnw_hbm, wq_hbm, wo_hbm, wg_hbm, wu_hbm, wd_hbm, k_hbm, v_hbm, out_ref,
           x_v, lnw_v, len_s, wq_v, wg_v, wu_v, k_v, v_v, wo_v, wd_v,
           q_b, mz_b, mg_b, ds_b, dr_b, y_b, z_b, of_b, f_b, xs_b, g_b,
           in_sem, wq_sem, gu_sem, k_sem, v_sem, w2_sem,
           q_ss, q_rs, mz_ss, mz_rs, mg_ss, mg_rs, d_ss, d_rs, y_ss, y_rs, z_ss, z_rs, x_ss, x_rs, g_ss, g_rs):
    xi = lax.axis_index('tp')
    sp = lax.axis_index('sp')
    c = lax.rem(sp, 2)
    y = lax.rem(lax.div(sp, 2), 4)
    z = lax.div(sp, 8)
    oc = 1 - c
    grp = y * 2 + c

    def dev(x_, z_, y_, c_):
        return (x_, (z_ * 4 + y_) * 2 + c_)

    def up(v, k):
        return lax.rem(v + k, 4)

    partner = dev(xi, z, y, oc)
    z_peers = [dev(xi, up(z, k), y, c) for k in (1, 2, 3)]
    y_peers = [dev(xi, z, up(y, k), c) for k in (1, 2, 3)]
    x_peers = [dev(up(xi, k), z, y, c) for k in (1, 2, 3)]
    yo_peers = [dev(xi, z, up(y, k), oc) for k in (1, 2, 3)]

    def start(src, dst, sem):
        cp = pltpu.make_async_copy(src, dst, sem)
        cp.start()
        return cp

    cp_x = start(x_hbm, x_v, in_sem.at[0])
    cp_lnw = start(lnw_hbm, lnw_v, in_sem.at[1])
    kc = HID // WQ_CHUNKS
    cp_wq = [start(wq_hbm.at[pl.ds(i * kc, kc), pl.ds(pl.multiple_of(c * 512, 512), 512)], wq_v.at[i], wq_sem.at[i])
             for i in range(WQ_CHUNKS)]

    bar = pltpu.get_barrier_semaphore()
    everyone = [partner] + z_peers + y_peers + x_peers + yo_peers
    for d in everyone:
        pl.semaphore_signal(bar, inc=1, device_id=d, device_id_type=MESH)

    ff = pl.multiple_of(jnp.minimum(z * 8 + grp, FF_BLOCKS - 1) * 128, 128)
    cp_g = start(wg_hbm.at[:, pl.ds(ff, 128)], wg_v, gu_sem.at[0])
    cp_u = start(wu_hbm.at[:, pl.ds(ff, 128)], wu_v, gu_sem.at[1])
    cp_len = start(len_hbm, len_s, in_sem.at[2])

    def row_of(j):
        return lax.rem(4 * oc + j, 8)

    def kv_copies(j):
        return (pltpu.make_async_copy(k_hbm.at[row_of(j)], k_v.at[j], k_sem.at[j]),
                pltpu.make_async_copy(v_hbm.at[row_of(j)], v_v.at[j], v_sem.at[j]))

    @pl.loop(0, 8)
    def _(j):
        for cp in kv_copies(j):
            cp.start()

    cols = pl.ds(pl.multiple_of(y * 1024, 1024), 1024)
    cp_k, cp_v = zip(*[kv_copies(j) for j in range(8)])

    sends = []

    def send(src, dst, ss, rs, d):
        cp = pltpu.make_async_remote_copy(src_ref=src, dst_ref=dst, send_sem=ss, recv_sem=rs,
                                          device_id=d, device_id_type=MESH)
        cp.start()
        sends.append(cp)

    def recv(dst, ss, rs, d):
        pltpu.make_async_remote_copy(src_ref=dst, dst_ref=dst, send_sem=ss, recv_sem=rs,
                                     device_id=d, device_id_type=MESH).wait_recv()

    cp_x.wait()
    cp_lnw.wait()
    xf = x_v[...].astype(F32)
    cen = xf - jnp.mean(xf, axis=-1, keepdims=True)
    var = jnp.mean(cen * cen, axis=-1, keepdims=True)
    h = (cen * lax.rsqrt(var + LN_EPS) * lnw_v[...].astype(F32).reshape(1, HID)).astype(BF16)

    q = jnp.zeros((ROWS, 512), F32)
    for i in range(WQ_CHUNKS):
        cp_wq[i].wait()
        q = q + jnp.dot(h[:, i * kc:(i + 1) * kc], wq_v[i], preferred_element_type=F32)
    q = q.astype(BF16).astype(F32)
    qrows = pl.ds(pl.multiple_of(c * 32, 32), 32)
    q_b[qrows, :] = jnp.concatenate([q[:, i * HD:(i + 1) * HD] for i in range(4)], axis=0)
    pl.semaphore_wait(bar, len(everyone))
    send(q_b.at[qrows, :], q_b.at[qrows, :], q_ss.at[0], q_rs.at[0], partner)

    cp_g.wait()
    cp_u.wait()
    gu = jnp.dot(h, jnp.concatenate([wg_v[...], wu_v[...]], axis=1), preferred_element_type=F32)
    act = (jax.nn.silu(gu[:, :HD]) * gu[:, HD:]).astype(BF16).astype(F32)
    mz_b[z] = act
    for k in (1, 2, 3):
        send(mz_b.at[z], mz_b.at[z], mz_ss.at[k - 1], mz_rs.at[z], z_peers[k - 1])

    prow = pl.ds(pl.multiple_of(oc * 32, 32), 32)
    recv(q_b.at[prow, :], q_ss.at[0], q_rs.at[0], partner)
    cp_len.wait()
    lane = lax.broadcasted_iota(jnp.int32, (ROWS, HD), 1)
    top = lax.broadcasted_iota(jnp.int32, (ROWS, HD), 0) < 4
    pos = sp * BLK + lax.broadcasted_iota(jnp.int32, (ROWS, BLK), 1)
    cs = (HD ** -0.5) * LOG2E

    def attend(js):
        for j in js:
            cp_k[j].wait()
        for j in js:
            cp_v[j].wait()
        ss = []
        for j in js:
            b = row_of(j)
            qh = q_b[pl.ds(b, 8, stride=8), :]
            qd = jnp.concatenate([jnp.where(top, qh, 0.0), jnp.where(top, 0.0, qh)], axis=1).astype(BF16)
            kk = jnp.concatenate([k_v[j, 0], k_v[j, 1]], axis=1)
            s = lax.dot_general(qd, kk, (((1,), (1,)), ((), ())), preferred_element_type=F32)
            ss.append(jnp.where(pos <= len_s[b], s, -jnp.inf))
        ms = [jnp.maximum(jnp.max(s, axis=-1, keepdims=True), NEG_BIG) for s in ss]
        ps = [jnp.exp2((s - m) * cs) for s, m in zip(ss, ms)]
        ls = [jnp.sum(p, axis=-1, keepdims=True) for p in ps]
        os = []
        for j, p in zip(js, ps):
            vv = jnp.concatenate([v_v[j, 0], v_v[j, 1]], axis=1)
            o2 = jnp.dot(p.astype(BF16), vv, preferred_element_type=F32)
            os.append(jnp.where(top, o2[:, :HD], o2[:, HD:]))
        return os, ms, ls

    def stats_tile(ms, ls):
        t = jnp.zeros((ROWS, HD), F32)
        for i in range(4):
            t = jnp.where(lane == i, ms[i], t)
            t = jnp.where(lane == 4 + i, ls[i], t)
        return t

    os, ms, ls = attend(range(4))
    for j in range(4):
        ds_b[j] = os[j]
    ds_b[4] = stats_tile(ms, ls)
    send(ds_b, dr_b, d_ss.at[0], d_rs.at[0], partner)
    cp_wo = start(wo_hbm.at[:, cols], wo_v, w2_sem.at[0])
    cp_wd = start(wd_hbm.at[:, cols], wd_v, w2_sem.at[1])
    own = list(zip(*attend(range(4, 8))))

    def combine(parts):
        mx = functools.reduce(jnp.maximum, [p[1] for p in parts])
        ws = [jnp.exp2((p[1] - mx) * cs) for p in parts]
        o = functools.reduce(jnp.add, [p[0] * w for p, w in zip(parts, ws)])
        l = functools.reduce(jnp.add, [p[2] * w for p, w in zip(parts, ws)])
        return o, mx, l

    def unpack(tile_of, i, st):
        return tile_of(i), st[:, i:i + 1], st[:, 4 + i:5 + i]

    recv(dr_b, d_ss.at[0], d_rs.at[0], partner)
    st = dr_b[4]
    ms, ls = [], []
    for i in range(4):
        o, m, l = combine([own[i], unpack(lambda r: dr_b[r], i, st)])
        y_b[y, i] = o
        ms.append(m)
        ls.append(l)
    y_b[y, 4] = stats_tile(ms, ls)
    for k in (1, 2, 3):
        send(y_b.at[y], y_b.at[y], y_ss.at[k - 1], y_rs.at[y], y_peers[k - 1])

    for k in (1, 2, 3):
        recv(mz_b.at[up(z, k)], mz_ss.at[k - 1], mz_rs.at[up(z, k)], z_peers[k - 1])
    mg_b[grp] = mz_b[...]
    gpeers = ([(partner, y * 2 + oc)] + [(y_peers[k - 1], up(y, k) * 2 + c) for k in (1, 2, 3)]
              + [(yo_peers[k - 1], up(y, k) * 2 + oc) for k in (1, 2, 3)])
    for n, (d, _) in enumerate(gpeers):
        send(mz_b, mg_b.at[grp], mg_ss.at[n], mg_rs.at[grp], d)

    for k in (1, 2, 3):
        recv(y_b.at[up(y, k)], y_ss.at[k - 1], y_rs.at[up(y, k)], y_peers[k - 1])
    ms, ls = [], []
    sts = [y_b[n, 4] for n in range(4)]
    for i in range(4):
        o, m, l = combine([unpack(lambda r, n=n: y_b[n, r], i, sts[n]) for n in range(4)])
        z_b[z, i] = o
        ms.append(m)
        ls.append(l)
    z_b[z, 4] = stats_tile(ms, ls)
    for k in (1, 2, 3):
        send(z_b.at[z], z_b.at[z], z_ss.at[k - 1], z_rs.at[z], z_peers[k - 1])

    for n, (d, g) in enumerate(gpeers):
        recv(mg_b.at[g], mg_ss.at[n], mg_rs.at[g], d)
    ml = jnp.concatenate([mg_b[i % 8, i // 8] for i in range(FF_BLOCKS)], axis=1).astype(BF16)
    cp_wd.wait()
    f_b[:, :512] = jnp.dot(ml, wd_v[:, :512], preferred_element_type=F32)
    f_b[:, 512:] = jnp.dot(ml, wd_v[:, 512:], preferred_element_type=F32)

    for k in (1, 2, 3):
        recv(z_b.at[up(z, k)], z_ss.at[k - 1], z_rs.at[up(z, k)], z_peers[k - 1])
    sts = [z_b[n, 4] for n in range(4)]
    for i in range(4):
        o, m, l = combine([unpack(lambda r, n=n: z_b[n, r], i, sts[n]) for n in range(4)])
        o = o / l
        of_b[pl.ds(i * 8, 8), :] = o
        of_b[pl.ds(32 + i * 8, 8), :] = o
    ol = jnp.concatenate([of_b[pl.ds(n, 8, stride=8), :] for n in range(8)], axis=1).astype(BF16)
    cp_wo.wait()
    r1 = f_b[:, :512] + jnp.dot(ol, wo_v[:, :512], preferred_element_type=F32)
    r2 = f_b[:, 512:] + jnp.dot(ol, wo_v[:, 512:], preferred_element_type=F32)

    upper = lax.broadcasted_iota(jnp.int32, (ROWS, 512), 0) < 4
    keep = jnp.logical_xor(upper, jnp.broadcast_to(c == 1, (ROWS, 512)))
    xs_b[xi] = jnp.where(keep, r1, pltpu.roll(r2, 4, 0))
    for k in (1, 2, 3):
        send(xs_b.at[xi], xs_b.at[xi], x_ss.at[k - 1], x_rs.at[xi], x_peers[k - 1])
    xc = x_v[:, pl.ds(pl.multiple_of(y * 1024, 1024), 1024)].astype(F32)
    xr = jnp.where(keep, xc[:, :512], pltpu.roll(xc[:, 512:], 4, 0))
    for k in (1, 2, 3):
        recv(xs_b.at[up(xi, k)], x_ss.at[k - 1], x_rs.at[up(xi, k)], x_peers[k - 1])
    tot = xr + ((xs_b[0] + xs_b[1]) + (xs_b[2] + xs_b[3]))
    g_b[grp] = tot.astype(BF16).astype(F32)
    for n, (d, _) in enumerate(gpeers):
        send(g_b.at[grp], g_b.at[grp], g_ss.at[n], g_rs.at[grp], d)
    for n, (d, g) in enumerate(gpeers):
        recv(g_b.at[g], g_ss.at[n], g_rs.at[g], d)
    for yy in range(4):
        a0, a1 = g_b[2 * yy], g_b[2 * yy + 1]
        out_ref[:, yy * 1024:yy * 1024 + 512] = jnp.where(upper, a0, a1).astype(BF16)
        out_ref[:, yy * 1024 + 512:yy * 1024 + 1024] = pltpu.roll(jnp.where(upper, a1, a0), 4, 0).astype(BF16)
    for cp in sends:
        cp.wait_send()


def solution(mesh):
    cache_spec = P(None, 'tp', 'sp', None)
    col_spec = P(None, 'tp')
    row_spec = P('tp', None)
    any_spec = pl.BlockSpec(memory_space=pl.ANY)
    dma = pltpu.SemaphoreType.DMA

    def local_step(*args):
        return pl.pallas_call(
            kernel,
            out_shape=pltpu.VMEM((ROWS, HID), BF16),
            in_specs=[any_spec] * 10,
            out_specs=pl.BlockSpec(memory_space=pltpu.VMEM),
            scratch_shapes=[
                pltpu.VMEM((ROWS, HID), BF16),
                pltpu.VMEM((HID,), BF16),
                pltpu.SMEM((ROWS,), jnp.int32),
                pltpu.VMEM((WQ_CHUNKS, HID // WQ_CHUNKS, 512), BF16),
                pltpu.VMEM((HID, HD), BF16),
                pltpu.VMEM((HID, HD), BF16),
                pltpu.VMEM((8, 2, BLK, HD), BF16),
                pltpu.VMEM((8, 2, BLK, HD), BF16),
                pltpu.VMEM((1024, 1024), BF16),
                pltpu.VMEM((3584, 1024), BF16),
                pltpu.VMEM((64, HD), F32),
                pltpu.VMEM((4, ROWS, HD), F32),
                pltpu.VMEM((8, 4, ROWS, HD), F32),
                pltpu.VMEM((5, ROWS, HD), F32),
                pltpu.VMEM((5, ROWS, HD), F32),
                pltpu.VMEM((4, 5, ROWS, HD), F32),
                pltpu.VMEM((4, 5, ROWS, HD), F32),
                pltpu.VMEM((64, HD), F32),
                pltpu.VMEM((ROWS, 1024), F32),
                pltpu.VMEM((4, ROWS, 512), F32),
                pltpu.VMEM((8, ROWS, 512), F32),
                dma((3,)), dma((WQ_CHUNKS,)), dma((2,)), dma((8,)), dma((8,)), dma((2,)),
                dma((1,)), dma((1,)),
                dma((3,)), dma((4,)),
                dma((7,)), dma((8,)),
                dma((1,)), dma((1,)),
                dma((3,)), dma((4,)),
                dma((3,)), dma((4,)),
                dma((3,)), dma((4,)),
                dma((7,)), dma((8,)),
            ],
            compiler_params=pltpu.CompilerParams(collective_id=0, has_side_effects=True,
                                                 vmem_limit_bytes=56 * 1024 * 1024),
        )(*args)

    return jax.shard_map(local_step, mesh=mesh,
                         in_specs=(P(), P(), P(), col_spec, row_spec,
                                   col_spec, col_spec, row_spec, cache_spec, cache_spec),
                         out_specs=P(), check_vma=False)
```
